32 devices in a mesh: seq: 8 (over z, x), fsdp: 4 (over y, core).
Axes of the slice: x: 2, y: 2, z: 4, core: 2. Of those that a mesh axis runs over, the one named last changes fastest.
Arguments:
- tokens: bfloat16 [4, 1024, 2048], P('fsdp', 'seq'), may hold values from -6 to 6
- cotangent: bfloat16 [4, 1024, 2048], P('fsdp', 'seq'), may hold values from -6 to 6
- routes: int32 [4, 1024, 8], P('fsdp', 'seq'), may hold values from 0 to 63, all different within a row; in each aligned block of 128 rows (0 to 127, 128 to 255, ..., all dimensions but the last counted through in order) at most 32 rows name the same one
- norm1_gain: bfloat16 [2048], P(('seq', 'fsdp')), may hold values from 0.099609375 to 1.8984375
- query_weight: bfloat16 [2048, 2048], P(('seq', 'fsdp')), may hold values from -0.125 to 0.125
- key_weight: bfloat16 [2048, 2048], P(('seq', 'fsdp')), may hold values from -0.125 to 0.125
- value_weight: bfloat16 [2048, 2048], P(('seq', 'fsdp')), may hold values from -0.125 to 0.125
- output_weight: bfloat16 [2048, 2048], P(('seq', 'fsdp')), may hold values from -2 to 2
- norm2_gain: bfloat16 [2048], P(('seq', 'fsdp')), may hold values from 0.099609375 to 1.8984375
- router_weight: bfloat16 [2048, 64], P(('seq', 'fsdp')), may hold values from -0.125 to 0.125
- expert_gate: bfloat16 [128, 2048, 512], P(('seq', 'fsdp')), may hold values from -0.125 to 0.125
- expert_up: bfloat16 [128, 2048, 512], P(('seq', 'fsdp')), may hold values from -0.125 to 0.125
- expert_down: bfloat16 [128, 512, 2048], P(('seq', 'fsdp')), may hold values from -0.75 to 0.75
Outputs:
- block_out: bfloat16 [4, 1024, 2048], P('fsdp', 'seq')
- input_grad: float32 [4, 1024, 2048], P('fsdp', 'seq')
- norm1_gain_grad: float32 [2048], P(('seq', 'fsdp'))
- query_weight_grad: float32 [2048, 2048], P(('seq', 'fsdp'))
- key_weight_grad: float32 [2048, 2048], P(('seq', 'fsdp'))
- value_weight_grad: float32 [2048, 2048], P(('seq', 'fsdp'))
- output_weight_grad: float32 [2048, 2048], P(('seq', 'fsdp'))
- norm2_gain_grad: float32 [2048], P(('seq', 'fsdp'))
- router_weight_grad: float32 [2048, 64], P(('seq', 'fsdp'))
- expert_gate_grad: float32 [128, 2048, 512], P(('seq', 'fsdp'))
- expert_up_grad: float32 [128, 2048, 512], P(('seq', 'fsdp'))
- expert_down_grad: float32 [128, 512, 2048], P(('seq', 'fsdp'))
The draws below stay inside these ranges and needn't reach their ends.
Inputs may be any that keep to these rules, and one draw needn't show every extreme that they name: `routes`: each row names 8 different experts. Among the 128 rows of one device (aligned blocks of the flattened sequences) no expert is named more than 32 times, and in every draw some expert is named exactly 32 times in some block; every expert is named somewhere.
All inputs are finite; a program needn't handle non-finite values.
Results may differ from the reference program's by a relative error of at most 0.02.
Values may be sent and summed in bfloat16 or wider, within the bound.
A program may use at most 448 MiB of HBM per device.

```python
import math
import jax
import jax.numpy as jnp
import numpy as np
from jax import lax

D = 2048
H = 16
HD = 128
E = 64
FF = 1024
TOP = 8
SPLIT = 2
TOK_DEV = 128
SEQ_LEN = 1024
SEQS = 4
CAP = 32
PIECES = 128
PIECE_FF = 512
N_SEQ = 8


def block_scale(own_key, shape, pieces, least, largest):
    def one(axis_at, parts):
        steps = jax.random.uniform(jax.random.fold_in(jax.random.fold_in(own_key, 6), axis_at), (parts,), jnp.float32, least / len(pieces), largest / len(pieces))
        return jnp.repeat(jnp.exp(steps), shape[axis_at] // parts).reshape((-1,) + (1,) * (len(shape) - axis_at - 1))

    factor_of = one(*pieces[0])
    for cut in pieces[1:]:
        factor_of = factor_of * one(*cut)
    return factor_of


def deal_out(rng, own, number, rows, count, top, most, skew):
    ranking = jax.random.permutation(rng, count)
    crowded, ordinary = portions_of(count, rows * top, most, skew, True), portions_of(count, rows * top, most, skew, False)
    places = jnp.arange(count)

    def named(sizes, rotation):
        used = int((sizes > 0).sum())
        fixed = max(1, used // 4)
        passed = fixed + (places - fixed + rotation * (used - fixed)) % max(1, count - fixed)
        return jnp.zeros((count,), jnp.int32).at[ranking[jnp.where(places < fixed, places, passed)]].set(jnp.asarray(sizes, jnp.int32))

    sizes = jnp.where(number % 4 == 0, named(crowded, number // 4), named(ordinary, number - number // 4 - 1))
    mixed = jax.random.permutation(jax.random.fold_in(own, 3), count)
    giver, receiver = mixed[0:count // 2 * 2:2], mixed[1:count // 2 * 2:2]
    room = jnp.minimum(sizes[giver] - 1, most - sizes[receiver]) // 2
    room = jnp.where((giver == ranking[0]) | (receiver == ranking[0]) | (sizes[receiver] == 0), 0, jnp.maximum(room, 0))
    passed = jax.random.randint(jax.random.fold_in(own, 4), (count // 2,), 0, 1 << 20) % (room + 1)
    sizes = sizes.at[giver].add(-passed).at[receiver].add(passed)
    labels = jnp.searchsorted(jnp.cumsum(sizes), jnp.arange(rows * top), side="right").astype(jnp.int32)
    listing = labels.reshape(top, rows).T
    listing = listing[jax.random.permutation(jax.random.fold_in(own, 1), rows)]
    rotation = jax.random.randint(jax.random.fold_in(own, 2), (rows, 1), 0, top)
    return jnp.take_along_axis(listing, (jnp.arange(top)[None, :] + rotation) % top, axis=1)


def portions_of(amount, total, reach, lean, full):
    portions = [(1 << 20) // math.isqrt(grade ** lean) + 1 for grade in range(1, amount + 1)]
    largest = reach if full else min(reach, max(-(-total // amount), total * portions[0] // sum(portions)))
    least = 1 if total - largest >= amount - 1 else 0
    counts, spare = [largest] + [least] * (amount - 1), total - largest - least * (amount - 1)
    while spare > 0:
        candidates = [i for i in range(1, amount) if counts[i] < largest] or [i for i in range(1, amount) if counts[i] < reach]
        mass, remaining = sum([portions[i] for i in candidates]), spare
        for i in candidates:
            addition = min(reach - counts[i], max(1, remaining * portions[i] // mass), spare)
            counts[i] = counts[i] + addition
            spare = spare - addition
    return np.array(counts)


def gaussian(stream_key, dims, deviation, reach, cuts=(), kind=jnp.bfloat16):
    result = deviation * jax.random.normal(stream_key, dims, jnp.float32)
    if cuts:
        result = result * block_scale(stream_key, dims, cuts, -0.22, 0.18)
    return jnp.clip(result, -reach, reach).astype(kind)


def setup_inputs(seed: int = 0) -> dict:
    arg_keys = jax.random.split(jax.random.key(seed), 14)
    tokens = gaussian(arg_keys[0], (SEQS, SEQ_LEN, D), 1.0, 6.0, ((0, 4), (1, 8)))
    cotangent = gaussian(arg_keys[1], (SEQS, SEQ_LEN, D), 1.0, 6.0, ((0, 4), (1, 8)))
    routes_keys = jax.random.split(jax.random.fold_in(arg_keys[2], 1), SEQS * SEQ_LEN // TOK_DEV)
    routes_turns = jax.random.permutation(jax.random.fold_in(arg_keys[2], 3), SEQS * SEQ_LEN // TOK_DEV)
    routes = jax.vmap(lambda own, number: deal_out(jax.random.fold_in(arg_keys[2], 2), own, number, TOK_DEV, E, TOP, CAP, 2))(routes_keys, routes_turns).reshape((SEQS, SEQ_LEN, TOP))
    norm1_gain = jnp.clip(1.0 + 0.18 * jax.random.normal(arg_keys[3], (D,), jnp.float32), 0.099609375, 1.8984375).astype(jnp.bfloat16)
    query_weight = gaussian(arg_keys[4], (D, D), D ** -0.5, 0.125, ((0, 32),))
    key_weight = gaussian(arg_keys[5], (D, D), D ** -0.5, 0.125, ((0, 32),))
    value_weight = gaussian(arg_keys[6], (D, D), D ** -0.5, 0.125, ((0, 32),))
    output_weight = gaussian(arg_keys[7], (D, D), (max(4 * D // SEQ_LEN, 1)) ** -0.5, 2.0, ((0, 32),))
    norm2_gain = jnp.clip(1.0 + 0.18 * jax.random.normal(arg_keys[8], (D,), jnp.float32), 0.099609375, 1.8984375).astype(jnp.bfloat16)
    router_weight = gaussian(arg_keys[9], (D, E), D ** -0.5, 0.125, ((0, 32),))
    expert_gate = gaussian(arg_keys[10], (PIECES, D, PIECE_FF), D ** -0.5, 0.125, ((0, 32),))
    expert_up = gaussian(arg_keys[11], (PIECES, D, PIECE_FF), D ** -0.5, 0.125, ((0, 32),))
    expert_down = gaussian(arg_keys[12], (PIECES, PIECE_FF, D), (FF // 16) ** -0.5, 0.75, ((0, 32),))
    return {"tokens": tokens, "cotangent": cotangent, "routes": routes, "norm1_gain": norm1_gain, "query_weight": query_weight, "key_weight": key_weight, "value_weight": value_weight, "output_weight": output_weight, "norm2_gain": norm2_gain, "router_weight": router_weight, "expert_gate": expert_gate, "expert_up": expert_up, "expert_down": expert_down}


epsilon = 1e-06
rope_base = 50000.0

def norm_rows(values, scales):
    mean_sq = lax.optimization_barrier(jnp.mean(values * values, axis=-1, keepdims=True))
    return values * lax.rsqrt(mean_sq + epsilon) * scales

def rope_tables(positions, head_dim):
    half_dim = head_dim // 2
    frequency = rope_base ** (-(2.0 * jnp.arange(half_dim, dtype=jnp.float32)) / head_dim)
    angles = positions.astype(jnp.float32)[:, None] * frequency[None, :]
    return (jnp.cos(angles), jnp.sin(angles))

def rotate(values, cosine, sine_tab, inverse):
    half_dim = values.shape[-1] // 2
    low_half = values[..., :half_dim]
    high_half = values[..., half_dim:]
    cos_rows = cosine[:, None, :]
    sin_rows = sine_tab[:, None, :]
    if inverse:
        return jnp.concatenate([low_half * cos_rows + high_half * sin_rows, high_half * cos_rows - low_half * sin_rows], axis=-1)
    return jnp.concatenate([low_half * cos_rows - high_half * sin_rows, high_half * cos_rows + low_half * sin_rows], axis=-1)

def log_sum_exp(scores):
    return jnp.log(lax.optimization_barrier(jnp.sum(jnp.exp(scores), axis=-1)))

def route_weights(logits, chosen):
    expo = jnp.exp(logits)
    probability = expo / lax.optimization_barrier(jnp.sum(expo, axis=-1, keepdims=True))
    picked = jnp.take_along_axis(probability, chosen, axis=-1)
    return picked / lax.optimization_barrier(jnp.sum(picked, axis=-1, keepdims=True))

def attend_forward(queries, keys_all, values_all):
    length, head_count, head_dim = queries.shape
    block_rows = min(512, length)
    score_scale = head_dim ** (-0.5)
    grouped = queries.reshape(length // block_rows, block_rows, head_count, head_dim)
    keys_wide = keys_all.astype(jnp.float32)
    values_wide = values_all.astype(jnp.float32)

    def one_block(query_block):
        scores = jnp.einsum('qhd,khd->hqk', query_block.astype(jnp.float32), keys_wide) * score_scale
        totals = log_sum_exp(scores)
        weights = jnp.exp(scores - totals[..., None]).astype(jnp.bfloat16)
        output = jnp.einsum('hqk,khd->qhd', weights.astype(jnp.float32), values_wide)
        return (output.astype(jnp.bfloat16), totals)
    outputs, totals = lax.map(one_block, grouped)
    return (outputs.reshape(length, head_count, head_dim), totals)

def attend_backward(queries, keys_all, values_all, outputs, totals, grad_out):
    length, head_count, head_dim = queries.shape
    block_rows = min(512, length)
    count_blocks = length // block_rows
    score_scale = head_dim ** (-0.5)
    keys_wide = keys_all.astype(jnp.float32)
    values_wide = values_all.astype(jnp.float32)

    def to_blocks(array):
        return array.reshape(count_blocks, block_rows, head_count, head_dim)

    def one_block(running, inputs):
        key_sum, value_sum = running
        query_block, output_block, grad_block, total_block = inputs
        grad_wide = grad_block.astype(jnp.float32)
        delta_rows = lax.optimization_barrier(jnp.sum(grad_wide * output_block.astype(jnp.float32), axis=-1))
        scores = jnp.einsum('qhd,khd->hqk', query_block.astype(jnp.float32), keys_wide) * score_scale
        weights = jnp.exp(scores - total_block[..., None])
        value_sum = value_sum + jnp.einsum('hqk,qhd->khd', weights.astype(jnp.bfloat16).astype(jnp.float32), grad_wide)
        weight_grad = jnp.einsum('qhd,khd->hqk', grad_wide, values_wide)
        score_grad = (weights * (weight_grad - delta_rows.T[:, :, None]) * score_scale).astype(jnp.bfloat16).astype(jnp.float32)
        query_grad = jnp.einsum('hqk,khd->qhd', score_grad, keys_wide).astype(jnp.bfloat16)
        key_sum = key_sum + jnp.einsum('hqk,qhd->khd', score_grad, query_block.astype(jnp.float32))
        return ((key_sum, value_sum), query_grad)
    zeros_kv = jnp.zeros(keys_all.shape, jnp.float32)
    (key_sum, value_sum), query_grad = lax.scan(one_block, (zeros_kv, zeros_kv), (to_blocks(queries), to_blocks(outputs), to_blocks(grad_out), totals))
    return (query_grad.reshape(length, head_count, head_dim), key_sum.astype(jnp.bfloat16), value_sum.astype(jnp.bfloat16))

def reference(tokens, cotangent, routes, norm1_gain, query_weight, key_weight, value_weight, output_weight, norm2_gain, router_weight, expert_gate, expert_up, expert_down):
    block_count = SEQS * N_SEQ
    gain_in = norm1_gain.astype(jnp.float32)
    gain_mid = norm2_gain.astype(jnp.float32)
    positions = jnp.arange(SEQ_LEN, dtype=jnp.int32)
    cosine, sine_tab = rope_tables(positions, HD)

    def forward_one(running, inputs):
        seq_tokens, seq_routes = inputs
        normed_in = norm_rows(seq_tokens.astype(jnp.float32), gain_in).astype(jnp.bfloat16)
        queries = rotate(jnp.dot(normed_in, query_weight, preferred_element_type=jnp.float32).reshape(SEQ_LEN, H, HD), cosine, sine_tab, False).astype(jnp.bfloat16)
        keys_all = rotate(jnp.dot(normed_in, key_weight, preferred_element_type=jnp.float32).reshape(SEQ_LEN, H, HD), cosine, sine_tab, False).astype(jnp.bfloat16)
        values_all = jnp.dot(normed_in, value_weight, preferred_element_type=jnp.float32).astype(jnp.bfloat16).reshape(SEQ_LEN, H, HD)
        attn_heads, totals = attend_forward(queries, keys_all, values_all)
        attn_rows = attn_heads.reshape(SEQ_LEN, D)
        residual = seq_tokens.astype(jnp.float32) + jnp.dot(attn_rows, output_weight, preferred_element_type=jnp.float32)
        normed_mid = norm_rows(residual, gain_mid).astype(jnp.bfloat16)
        logits = jnp.dot(normed_mid, router_weight, preferred_element_type=jnp.float32)
        weights = route_weights(logits, seq_routes)
        return (running, (normed_in, queries, keys_all, values_all, attn_heads, totals, residual, normed_mid, logits, weights))
    _, saved = lax.scan(forward_one, jnp.zeros((), jnp.float32), (tokens, routes))
    total_rows = SEQS * SEQ_LEN
    route_count = total_rows * TOP
    flat_routes = routes.reshape(block_count, TOK_DEV * TOP)
    onehot = (flat_routes[..., None] == jnp.arange(E, dtype=jnp.int32)).astype(jnp.int32)
    before = jnp.cumsum(onehot, axis=1) - onehot
    slot_pos = lax.optimization_barrier(jnp.sum(before * onehot, axis=-1))
    slot_index = flat_routes * (block_count * CAP) + jnp.arange(block_count, dtype=jnp.int32)[:, None] * CAP + slot_pos
    route_ids = jnp.full((E * block_count * CAP,), route_count, jnp.int32).at[slot_index.reshape(-1)].set(jnp.arange(route_count, dtype=jnp.int32))
    route_ids = route_ids.reshape(E, block_count * CAP)
    normed_all = jnp.concatenate([saved[7].reshape(total_rows, D), jnp.zeros((1, D), jnp.bfloat16)], axis=0)
    cot_all = jnp.concatenate([cotangent.reshape(total_rows, D).astype(jnp.float32), jnp.zeros((1, D), jnp.float32)], axis=0)
    weight_all = jnp.concatenate([saved[9].reshape(-1), jnp.zeros((1,), jnp.float32)], axis=0)
    gate_parts = expert_gate.reshape(E, SPLIT, D, PIECE_FF)
    up_parts = expert_up.reshape(E, SPLIT, D, PIECE_FF)
    down_parts = expert_down.reshape(E, SPLIT, PIECE_FF, D)

    def expert_step(running, inputs):
        moe_sum, weight_grad, normed_grad = running
        slot_ids, gate_piece, up_piece, down_piece = inputs
        token_ids = slot_ids // TOP
        rows_in = normed_all[token_ids]
        route_w = weight_all[slot_ids]
        cot_rows = cot_all[token_ids]
        rows_grad = (route_w[:, None] * cot_rows).astype(jnp.bfloat16)
        total_out = jnp.zeros((block_count * CAP, D), jnp.float32)
        total_back = jnp.zeros((block_count * CAP, D), jnp.float32)
        grad_gates = []
        grad_ups = []
        grad_downs = []
        for piece_index in range(SPLIT):
            pre_gate = jnp.dot(rows_in, gate_piece[piece_index], preferred_element_type=jnp.float32)
            pre_up = jnp.dot(rows_in, up_piece[piece_index], preferred_element_type=jnp.float32)
            gate_sigmoid = jax.nn.sigmoid(pre_gate)
            active = pre_gate * gate_sigmoid
            hidden = (active * pre_up).astype(jnp.bfloat16)
            piece_out = jnp.dot(hidden, down_piece[piece_index], preferred_element_type=jnp.float32).astype(jnp.bfloat16)
            total_out = total_out + lax.optimization_barrier(piece_out).astype(jnp.float32)
            hidden_grad = jnp.dot(rows_grad, down_piece[piece_index].T, preferred_element_type=jnp.float32)
            grad_downs.append(jnp.dot(hidden.T, rows_grad, preferred_element_type=jnp.float32))
            gate_grad = (hidden_grad * pre_up * gate_sigmoid * (1.0 + pre_gate * (1.0 - gate_sigmoid))).astype(jnp.bfloat16)
            up_grad = (hidden_grad * active).astype(jnp.bfloat16)
            grad_gates.append(jnp.dot(rows_in.T, gate_grad, preferred_element_type=jnp.float32))
            grad_ups.append(jnp.dot(rows_in.T, up_grad, preferred_element_type=jnp.float32))
            back_part = jnp.dot(gate_grad, gate_piece[piece_index].T, preferred_element_type=jnp.float32) + jnp.dot(up_grad, up_piece[piece_index].T, preferred_element_type=jnp.float32)
            total_back = total_back + lax.optimization_barrier(back_part.astype(jnp.bfloat16)).astype(jnp.float32)
        moe_sum = moe_sum.at[token_ids].add(route_w[:, None] * total_out, mode='drop')
        weight_grad = weight_grad.at[slot_ids].add(lax.optimization_barrier(jnp.sum(cot_rows * total_out, axis=-1)), mode='drop')
        normed_grad = normed_grad.at[token_ids].add(total_back, mode='drop')
        return ((moe_sum, weight_grad, normed_grad), (jnp.stack(grad_gates), jnp.stack(grad_ups), jnp.stack(grad_downs)))
    start_state = (jnp.zeros((total_rows, D), jnp.float32), jnp.zeros((route_count,), jnp.float32), jnp.zeros((total_rows, D), jnp.float32))
    (moe_sum, weight_grad, normed_grad), (gate_grads, up_grads, down_grads) = lax.scan(expert_step, start_state, (route_ids, gate_parts, up_parts, down_parts))

    def backward_one(running, inputs):
        normed_in, queries, keys_all, values_all, attn_heads, totals, residual, normed_mid, logits, weights, seq_tokens, seq_routes, seq_cot, moe_part, seq_wgrad, seq_ngrad = inputs
        grad_q, grad_k, grad_v, grad_o, grad_r, grad_g1, grad_g2 = running
        block_out = (residual + moe_part).astype(jnp.bfloat16)
        _, route_back = jax.vjp(lambda values: route_weights(values, seq_routes), logits)
        logit_grad = route_back(seq_wgrad)[0].astype(jnp.bfloat16)
        normed_total = seq_ngrad + jnp.dot(logit_grad, router_weight.T, preferred_element_type=jnp.float32)
        grad_r = grad_r + jnp.dot(normed_mid.T, logit_grad, preferred_element_type=jnp.float32)
        _, norm_back = jax.vjp(norm_rows, residual, gain_mid)
        resid_part, gain_mid_grad = norm_back(normed_total)
        grad_g2 = grad_g2 + gain_mid_grad
        resid_grad = seq_cot.astype(jnp.float32) + resid_part
        resid_round = resid_grad.astype(jnp.bfloat16)
        attn_rows = attn_heads.reshape(SEQ_LEN, D)
        grad_o = grad_o + jnp.dot(attn_rows.T, resid_round, preferred_element_type=jnp.float32)
        attn_grad = jnp.dot(resid_round, output_weight.T, preferred_element_type=jnp.float32).astype(jnp.bfloat16).reshape(SEQ_LEN, H, HD)
        query_grad, key_grad, value_grad = attend_backward(queries, keys_all, values_all, attn_heads, totals, attn_grad)
        query_rows = rotate(query_grad.astype(jnp.float32), cosine, sine_tab, True).astype(jnp.bfloat16).reshape(SEQ_LEN, D)
        key_rows = rotate(key_grad.astype(jnp.float32), cosine, sine_tab, True).astype(jnp.bfloat16).reshape(SEQ_LEN, D)
        value_rows = value_grad.reshape(SEQ_LEN, D)
        grad_q = grad_q + jnp.dot(normed_in.T, query_rows, preferred_element_type=jnp.float32)
        grad_k = grad_k + jnp.dot(normed_in.T, key_rows, preferred_element_type=jnp.float32)
        grad_v = grad_v + jnp.dot(normed_in.T, value_rows, preferred_element_type=jnp.float32)
        normed_in_grad = jnp.dot(query_rows, query_weight.T, preferred_element_type=jnp.float32) + jnp.dot(key_rows, key_weight.T, preferred_element_type=jnp.float32) + jnp.dot(value_rows, value_weight.T, preferred_element_type=jnp.float32)
        _, norm_back_in = jax.vjp(norm_rows, seq_tokens.astype(jnp.float32), gain_in)
        input_part, gain_in_grad = norm_back_in(normed_in_grad)
        grad_g1 = grad_g1 + gain_in_grad
        input_grad = resid_grad + input_part
        return ((grad_q, grad_k, grad_v, grad_o, grad_r, grad_g1, grad_g2), (block_out, input_grad))
    zero_dd = jnp.zeros((D, D), jnp.float32)
    grad_state = (zero_dd, zero_dd, zero_dd, zero_dd, jnp.zeros((D, E), jnp.float32), jnp.zeros((D,), jnp.float32), jnp.zeros((D,), jnp.float32))
    back_inputs = saved + (tokens, routes, cotangent, moe_sum.reshape(SEQS, SEQ_LEN, D), weight_grad.reshape(SEQS, SEQ_LEN, TOP), normed_grad.reshape(SEQS, SEQ_LEN, D))
    grads, (block_out, input_grad) = lax.scan(backward_one, grad_state, back_inputs)
    grad_q, grad_k, grad_v, grad_o, grad_r, grad_g1, grad_g2 = grads
    return (block_out, input_grad, grad_g1, grad_q, grad_k, grad_v, grad_o, grad_g2, grad_r, gate_grads.reshape(PIECES, D, PIECE_FF), up_grads.reshape(PIECES, D, PIECE_FF), down_grads.reshape(PIECES, PIECE_FF, D))
```

```python
import jax
import jax.numpy as jnp
from jax import lax
from jax.sharding import PartitionSpec as P

H = 16
HD = 128
SPLIT = 2
AXES = ("seq", "fsdp")

epsilon = 1e-06
rope_base = 50000.0
bf16 = jnp.bfloat16
f32 = jnp.float32


def norm_rows(values, scales):
    mean_sq = jnp.mean(values * values, axis=-1, keepdims=True)
    return values * lax.rsqrt(mean_sq + epsilon) * scales


def rope_tables(positions, head_dim):
    half_dim = head_dim // 2
    frequency = rope_base ** (-(2.0 * jnp.arange(half_dim, dtype=f32)) / head_dim)
    angles = positions.astype(f32)[:, None] * frequency[None, :]
    return (jnp.cos(angles), jnp.sin(angles))


def rotate(values, cosine, sine_tab, inverse):
    half_dim = values.shape[-1] // 2
    low_half = values[..., :half_dim]
    high_half = values[..., half_dim:]
    cos_rows = cosine[:, None, :]
    sin_rows = -sine_tab[:, None, :] if inverse else sine_tab[:, None, :]
    return jnp.concatenate(
        [low_half * cos_rows - high_half * sin_rows, high_half * cos_rows + low_half * sin_rows],
        axis=-1,
    )


def route_weights(logits, chosen):
    expo = jnp.exp(logits)
    probability = expo / jnp.sum(expo, axis=-1, keepdims=True)
    experts = jnp.arange(logits.shape[1], dtype=jnp.int32)
    match = (chosen[:, :, None] == experts).astype(f32)
    picked = jnp.sum(match * probability[:, None, :], axis=-1)
    return picked / jnp.sum(picked, axis=-1, keepdims=True)


def mm(left, right):
    return jnp.dot(left, right, preferred_element_type=f32)


def mm_tn(left, right):
    return lax.dot_general(left, right, (((0,), (0,)), ((), ())), preferred_element_type=f32)


def mm_nt(left, right):
    return lax.dot_general(left, right, (((1,), (1,)), ((), ())), preferred_element_type=f32)


def ein(spec, *args):
    return jnp.einsum(spec, *args, preferred_element_type=f32)


def body(
    tokens,
    cotangent,
    routes,
    norm1_gain,
    query_weight,
    key_weight,
    value_weight,
    output_weight,
    norm2_gain,
    router_weight,
    expert_gate,
    expert_up,
    expert_down,
):
    n_seq = lax.axis_size("seq")
    n_fsdp = lax.axis_size("fsdp")
    n_dev = n_seq * n_fsdp
    seq_at = lax.axis_index("seq")
    dev_at = seq_at * n_fsdp + lax.axis_index("fsdp")
    tok_rows, width = tokens.shape[1], tokens.shape[2]
    length = tok_rows * n_seq
    heads = H // n_seq
    cols = heads * HD
    shard = query_weight.shape[0]
    experts = router_weight.shape[1]
    top_k = routes.shape[2]
    capacity = tok_rows * top_k // experts * 2
    pieces = expert_gate.shape[0]
    n_loc = max(1, pieces // SPLIT)
    per_loc = pieces // n_loc
    first_expert = dev_at * pieces // SPLIT

    x_own = tokens[0]
    cot_own = cotangent[0]
    chosen = routes[0]

    routes_all = lax.all_gather(chosen, AXES, axis=0, tiled=True)
    x_seq = lax.all_gather(x_own, "seq", axis=0, tiled=True)
    small = jnp.concatenate(
        [
            router_weight,
            norm1_gain[:, None],
            norm2_gain[:, None],
            jnp.zeros((shard, 128 - experts - 2), bf16),
        ],
        axis=1,
    )
    blocks = jnp.concatenate(
        [
            query_weight.reshape(shard, n_seq, cols),
            key_weight.reshape(shard, n_seq, cols),
            value_weight.reshape(shard, n_seq, cols),
            jnp.broadcast_to(small[:, None, :], (shard, n_seq, 128)),
        ],
        axis=2,
    ).transpose(1, 0, 2)
    moved = lax.all_to_all(blocks, "seq", split_axis=0, concat_axis=0, tiled=True)
    packed = lax.all_gather(moved, "fsdp", axis=1).reshape(width, 3 * cols + 128)
    w_qkv = packed[:, : 3 * cols]
    router_full = packed[:, 3 * cols : 3 * cols + experts]
    gain_in = packed[:, 3 * cols + experts].astype(f32)
    gain_mid = packed[:, 3 * cols + experts + 1].astype(f32)
    out_full = lax.all_gather(output_weight, AXES, axis=0, tiled=True)
    out_rows = lax.dynamic_slice_in_dim(out_full, seq_at * cols, cols, 0)
    cot_all = lax.all_gather(cot_own, AXES, axis=0, tiled=True)

    cosine, sine_tab = rope_tables(jnp.arange(length, dtype=jnp.int32), HD)
    normed_in = norm_rows(x_seq.astype(f32), gain_in).astype(bf16)
    qkv = mm(normed_in, w_qkv)
    q = rotate(qkv[:, :cols].reshape(length, heads, HD), cosine, sine_tab, False).astype(bf16)
    k = rotate(qkv[:, cols : 2 * cols].reshape(length, heads, HD), cosine, sine_tab, False).astype(bf16)
    v = qkv[:, 2 * cols :].astype(bf16).reshape(length, heads, HD)
    scale = HD ** (-0.5)
    scores = ein("qhd,khd->hqk", q, k) * scale
    totals = jnp.log(jnp.sum(jnp.exp(scores), axis=-1))
    probs = jnp.exp(scores - totals[..., None])
    attn_heads = ein("hqk,khd->qhd", probs.astype(bf16), v).astype(bf16)
    attn_flat = attn_heads.reshape(length, cols)
    attn_rows = lax.all_to_all(attn_flat, "seq", split_axis=0, concat_axis=1, tiled=True)

    x_own32 = x_own.astype(f32)
    residual = x_own32 + mm(attn_rows, out_full)
    normed_mid = norm_rows(residual, gain_mid).astype(bf16)

    x_all = lax.all_gather(normed_mid, AXES, axis=0, tiled=True)
    logits_all = mm(x_all, router_full)
    w_all = route_weights(logits_all, routes_all)

    local = first_expert + jnp.arange(n_loc, dtype=jnp.int32)
    match = routes_all.reshape(n_dev, tok_rows, top_k)[:, None] == local[None, :, None, None]
    hit = jnp.any(match, axis=-1)
    w_hit = jnp.sum(jnp.where(match, w_all.reshape(n_dev, 1, tok_rows, top_k), 0.0), axis=-1)
    tri = (jnp.arange(tok_rows)[:, None] <= jnp.arange(tok_rows)[None, :]).astype(bf16)
    place = ein("bet,tu->beu", hit.astype(bf16), tri).astype(jnp.int32) - 1
    slots = jnp.arange(capacity, dtype=jnp.int32)
    pick = hit[:, :, None, :] & (place[:, :, None, :] == slots[None, None, :, None])
    one = pick.astype(bf16)
    w_slot = jnp.sum(jnp.where(pick, w_hit[:, :, None, :], 0.0), axis=-1)
    rows_of = lambda a: ein("best,btd->ebsd", one, a.reshape(n_dev, tok_rows, width)).reshape(
        n_loc, n_dev * capacity, width
    )
    rows_in = rows_of(x_all).astype(bf16)
    rows_cot = rows_of(cot_all)
    w_rows = w_slot.transpose(1, 0, 2).reshape(n_loc, n_dev * capacity, 1)
    rows_grad = (w_rows * rows_cot).astype(bf16)
    gate = expert_gate.reshape(n_loc, per_loc, width, -1)
    up = expert_up.reshape(n_loc, per_loc, width, -1)
    down = expert_down.reshape(n_loc, per_loc, -1, width)

    pre_gate = ein("erd,epdf->eprf", rows_in, gate)
    pre_up = ein("erd,epdf->eprf", rows_in, up)
    sig = jax.nn.sigmoid(pre_gate)
    active = pre_gate * sig
    hidden = (active * pre_up).astype(bf16)
    hidden_grad = ein("erd,epfd->eprf", rows_grad, down)
    gate_grad = (hidden_grad * pre_up * sig * (1.0 + pre_gate * (1.0 - sig))).astype(bf16)
    up_grad = (hidden_grad * active).astype(bf16)
    back = ein("eprf,epdf->erd", gate_grad, gate) + ein("eprf,epdf->erd", up_grad, up)
    out = ein("eprf,epfd->erd", hidden, down)
    w_back = jnp.sum(rows_cot * out, axis=-1)
    spread = lambda a: ein(
        "best,ebsd->btd", one, a.astype(bf16).reshape(n_loc, n_dev, capacity, width)
    ).astype(bf16).reshape(n_dev * tok_rows, width)
    back_own = lax.psum_scatter(spread(back), AXES, scatter_dimension=0, tiled=True)
    w_tok = jnp.sum(
        jnp.where(pick, w_back.reshape(n_loc, n_dev, capacity).transpose(1, 0, 2)[..., None], 0.0), axis=2
    )
    w_parts = lax.all_to_all(w_tok, AXES, split_axis=0, concat_axis=0, tiled=True)
    w_by_expert = w_parts.reshape(experts, n_dev * n_loc // experts, tok_rows).sum(axis=1)
    own_match = (chosen[:, :, None] == jnp.arange(experts, dtype=jnp.int32)).astype(f32)
    weight_grad = jnp.sum(own_match * w_by_expert.T[:, None, :], axis=-1)
    moe_own = lax.psum_scatter(spread(w_rows * out), AXES, scatter_dimension=0, tiled=True)
    block_out = (residual + moe_own.astype(f32)).astype(bf16)

    down_grad = ein("eprf,erd->epfd", hidden, rows_grad).reshape(expert_down.shape)
    gate_weight_grad = ein("erd,eprf->epdf", rows_in, gate_grad).reshape(expert_gate.shape)
    up_weight_grad = ein("erd,eprf->epdf", rows_in, up_grad).reshape(expert_up.shape)

    logits = mm(normed_mid, router_full)
    _, route_back = jax.vjp(lambda values: route_weights(values, chosen), logits)
    logit_grad = route_back(weight_grad)[0].astype(bf16)
    normed_total = back_own.astype(f32) + mm_nt(logit_grad, router_full)
    logit_all = lax.all_gather(logit_grad, AXES, axis=0, tiled=True)
    x_cols = lax.dynamic_slice_in_dim(x_all, dev_at * shard, shard, 1)
    grad_router = mm_tn(x_cols, logit_all)
    cot32 = cot_own.astype(f32)
    _, norm_back = jax.vjp(norm_rows, residual, gain_mid)
    resid_part, gain_two = norm_back(normed_total)
    resid_grad = cot32 + resid_part
    resid_seq = lax.all_gather(resid_grad.astype(bf16), "seq", axis=0, tiled=True)

    grad_out_rows = mm_tn(attn_flat, resid_seq)
    grad_output = lax.psum_scatter(grad_out_rows, "fsdp", scatter_dimension=0, tiled=True)
    attn_grad = mm_nt(resid_seq, out_rows).astype(bf16).reshape(length, heads, HD)
    delta = jnp.sum(attn_grad.astype(f32) * attn_heads.astype(f32), axis=-1)
    v_grad = ein("hqk,qhd->khd", probs.astype(bf16), attn_grad).astype(bf16)
    p_grad = ein("qhd,khd->hqk", attn_grad, v)
    s_grad = (probs * (p_grad - delta.T[:, :, None]) * scale).astype(bf16)
    q_grad = ein("hqk,khd->qhd", s_grad, k).astype(bf16)
    k_grad = ein("hqk,qhd->khd", s_grad, q).astype(bf16)
    q_rows = rotate(q_grad.astype(f32), cosine, sine_tab, True).astype(bf16)
    k_rows = rotate(k_grad.astype(f32), cosine, sine_tab, True).astype(bf16)
    d_qkv = jnp.concatenate([a.reshape(length, cols) for a in (q_rows, k_rows, v_grad)], axis=1)
    in_part = mm_nt(d_qkv, w_qkv).astype(bf16)
    normed_in_grad = lax.psum_scatter(in_part, "seq", scatter_dimension=0, tiled=True).astype(f32)
    _, norm_back_in = jax.vjp(norm_rows, x_own32, gain_in)
    input_part, gain_one = norm_back_in(normed_in_grad)
    input_grad = resid_grad + input_part

    grad_qkv = mm_tn(normed_in, d_qkv).reshape(n_seq, n_fsdp, shard, 3 * cols)
    grad_qkv = lax.psum_scatter(grad_qkv, "fsdp", scatter_dimension=1, tiled=False)
    grad_qkv = lax.all_to_all(grad_qkv, "seq", split_axis=0, concat_axis=0, tiled=True)
    grad_qkv = grad_qkv.reshape(n_seq, shard, 3, cols).transpose(2, 1, 0, 3).reshape(3, shard, width)
    gains = lax.psum_scatter(
        jnp.stack([gain_one, gain_two]).reshape(2, n_dev, shard), AXES, scatter_dimension=1, tiled=False
    )
    return (
        block_out[None],
        input_grad[None],
        gains[0],
        grad_qkv[0],
        grad_qkv[1],
        grad_qkv[2],
        grad_output,
        gains[1],
        grad_router,
        gate_weight_grad,
        up_weight_grad,
        down_grad,
    )


def solution(mesh):
    rows3 = P("fsdp", "seq", None)
    flat = P(AXES)
    two = P(AXES, None)
    three = P(AXES, None, None)
    return jax.shard_map(
        body,
        mesh=mesh,
        in_specs=(rows3, rows3, rows3, flat, two, two, two, two, flat, two, three, three, three),
        out_specs=(rows3, rows3, flat, two, two, two, two, flat, two, three, three, three),
        check_vma=False,
    )
```
